32 devices in a mesh: blk: 16 (over z, y, x), ga: 2 (over core).
Axes of the slice: x: 2, y: 2, z: 4, core: 2. Of those that a mesh axis runs over, the one named last changes fastest.
Arguments:
- pair_elements: bfloat16 [4096, 16384], P('ga', 'blk'), may hold values from -6 to 6
- screening: bfloat16 [4096, 4096], P('ga', 'blk'), may hold values from -0.09375 to 0.09375
- energies: float32 [256], replicated, may hold values from 0.5 to 3
- frequencies: float32 [8], replicated, may hold values from 0.3 to 3
- qp_index: int32 [32], replicated, may hold values from 0 to 255
- occupied: int32 [256], replicated, may hold values 0 or 1
Outputs:
- self_energy: float32 [2, 8, 32, 32], replicated
The draws below stay inside these ranges and needn't reach their ends.
All inputs are finite; a program needn't handle non-finite values.
Results may differ from the reference program's by a relative error of at most 0.0003.
Values may be sent and summed in bfloat16 or wider, within the bound.
A program may use at most 128 MiB of HBM per device.

```python
import math
import jax
import jax.numpy as jnp
from jax import lax

STATES = 32
BAND_DEV = 16
NG = 4096
NFREQ = 8
NB = 256


def set_ends(values, stream_key, least, top_value):
    longest = values.shape.index(max(values.shape))
    spots = []
    for shift in (0, 1):
        where = [jax.random.randint(jax.random.fold_in(stream_key, axis), (), 0, length) for axis, length in enumerate(values.shape)]
        where[longest] = (where[longest] + shift) % values.shape[longest]
        spots.append(tuple(where))
    return values.at[spots[0]].set(least).at[spots[1]].set(top_value)


def level_of(stream_key, extent, cuts, least, top_value):
    level, own = 1.0, jax.random.fold_in(stream_key, 6)
    for axis_at, blocks in cuts:
        heights = jnp.exp(jax.random.uniform(jax.random.fold_in(own, axis_at), (blocks,), jnp.float32, least / len(cuts), top_value / len(cuts)))
        level = level * jnp.repeat(heights, extent[axis_at] // blocks).reshape([-1 if axis == axis_at else 1 for axis in range(len(extent))])
    return level


def centred(rng, dims, scale, reach, cuts=(), kind=jnp.bfloat16):
    gain = level_of(rng, dims, cuts, -0.22, 0.18) if cuts else 1.0
    entries = jax.random.normal(rng, dims, jnp.float32) * scale * gain
    return jnp.minimum(jnp.maximum(entries, -reach), reach).astype(kind)


def setup_inputs(seed: int = 0) -> dict:
    key_list = jax.random.split(jax.random.key(seed), 7)
    pair_elements = centred(key_list[0], (NG, NB * 2 * STATES), 1.0, 6.0, ((0, 2), (1, 16)))
    screening = centred(key_list[1], (NG, NG), NG ** -0.5, 0.09375, ((0, 2), (1, 16)))
    energies = jnp.clip(jax.random.uniform(key_list[2], (NB,), jnp.float32, 0.5, 3.0), 0.5, 3.0)
    frequencies = jnp.clip(jnp.exp(jax.random.uniform(key_list[3], (NFREQ,), jnp.float32, math.log(0.3), math.log(3.0))), 0.3, 3.0)
    qp_index = set_ends(jax.random.randint(key_list[4], (STATES,), 0, NB), jax.random.fold_in(key_list[4], 1), 0, NB - 1).astype(jnp.int32)
    occupied = set_ends((jax.random.randint(key_list[5], (NB,), 0, 2) < 1).astype(jnp.int32), jax.random.fold_in(key_list[5], 1), 0, 1)
    return {"pair_elements": pair_elements, "screening": screening, "energies": energies, "frequencies": frequencies, "qp_index": qp_index, "occupied": occupied}


def band_weights(energies, frequencies, qp_index, occupied, offset, band_count):
    level_count = energies.shape[0]
    position = jnp.arange(level_count, dtype=jnp.int32)
    signed = jnp.where(occupied == 1, -energies, energies)
    onehot = (qp_index[:, None] == position[None, :]).astype(jnp.float32)
    state_level = jnp.sum(onehot * signed[None, :], axis=1)
    band_level = lax.dynamic_slice_in_dim(signed, offset, band_count, 0)
    detuning = state_level[:, None] - band_level[None, :]
    imag_freq = frequencies[:, None, None]
    modulus = detuning[None] ** 2 + imag_freq ** 2
    return detuning[None] / modulus, -imag_freq / modulus


def window_sigma(elements, screened, weight_real, weight_imag, band_count):
    row_count = elements.shape[0]
    local_elems = elements.astype(jnp.float32).reshape(row_count, band_count, 2, STATES)
    image_cols = screened.reshape(row_count, band_count, 2, STATES)
    intersection = jnp.einsum("gnpi,gnqj->npiqj", local_elems, image_cols, precision=lax.Precision.HIGHEST)
    intersection_real = intersection[:, 0, :, 0, :] + intersection[:, 1, :, 1, :]
    intersection_imag = intersection[:, 0, :, 1, :] - intersection[:, 1, :, 0, :]
    sigma_real = jnp.einsum("kin,nij->kij", weight_real, intersection_real, precision=lax.Precision.HIGHEST) - jnp.einsum("kin,nij->kij", weight_imag, intersection_imag, precision=lax.Precision.HIGHEST)
    sigma_imag = jnp.einsum("kin,nij->kij", weight_real, intersection_imag, precision=lax.Precision.HIGHEST) + jnp.einsum("kin,nij->kij", weight_imag, intersection_real, precision=lax.Precision.HIGHEST)
    return jnp.stack([sigma_real, sigma_imag]) / NG


def reference(pair_elements, screening, energies, frequencies, qp_index, occupied):
    window_count = energies.shape[0] // BAND_DEV
    col_count = BAND_DEV * 2 * STATES

    def band_window(window_index):
        column_start = (window_index * col_count).astype(jnp.int32)
        elements = lax.dynamic_slice_in_dim(pair_elements, column_start, col_count, 1)
        screened = jnp.dot(screening, elements, preferred_element_type=jnp.float32)
        band_start = (window_index * BAND_DEV).astype(jnp.int32)
        weight_real, weight_imag = band_weights(energies, frequencies, qp_index, occupied, band_start, BAND_DEV)
        return window_sigma(elements, screened, weight_real, weight_imag, BAND_DEV)

    windows = lax.map(band_window, jnp.arange(window_count, dtype=jnp.int32))
    return jnp.sum(windows, axis=0)
```

```python
import functools

import jax
import jax.numpy as jnp
from jax import lax
from jax.experimental import pallas as pl
from jax.experimental.pallas import tpu as pltpu
from jax.sharding import PartitionSpec as P

MESH = pl.DeviceIdType.MESH
CHUNKS = 8


def sigma_kernel(
    n, ga, bw, m_ref, w_ref, a_ref, mbuf, wbuf, wx, s, lsem,
    wxs, wxr, mxs, mxr, mos, mor, mrs, mrr, wzs, wzr, wys, wyr,
):
    rows, cols = m_ref.shape
    half = rows // 2
    kc = w_ref.shape[1]
    nz = n // 4
    cr = rows // CHUNKS
    b, g = lax.axis_index("blk"), lax.axis_index("ga")
    x, y, z = b % 2, (b // 2) % 2, b // 4
    px = b + 1 - 2 * x
    py = b + 2 - 4 * y

    def remote(src, dst, ss, rs, dev):
        return pltpu.make_async_remote_copy(
            src_ref=src, dst_ref=dst, send_sem=ss, recv_sem=rs, device_id=dev, device_id_type=MESH
        )

    def piece(zz, yy, xx):
        return zz * 4 + yy * 2 + xx

    def side(kind):
        return x if kind == 0 else 1 - x

    def w_x():
        return remote(wx, wbuf.at[b], wxs, wxr, (px, g))

    def w_x_in():
        return remote(wx, wbuf.at[px], wxs, wxr, (px, g))

    def w_z(kind, k):
        blk = wbuf.at[piece(z, y, side(kind))]
        return remote(blk, blk, wzs.at[kind, k], wzr.at[kind, k], (piece((z + k) % nz, y, x), g))

    def w_z_in(kind, k):
        blk = wbuf.at[piece((z + nz - k) % nz, y, side(kind))]
        return remote(blk, blk, wzs.at[kind, k], wzr.at[kind, k], (piece((z + k) % nz, y, x), g))

    def w_y(kind, k, row):
        blk = wbuf.at[piece((z + nz - k) % nz, row, side(kind))]
        return remote(blk, blk, wys.at[kind, k], wyr.at[kind, k], (py, g))

    def m_x(c):
        at = pl.ds(pl.multiple_of(g * rows + c * cr, cr), cr)
        return remote(mbuf.at[0, at], mbuf.at[1, at], mxs.at[c], mxr.at[c], (px, g))

    def m_own(k, who):
        blk = mbuf.at[0, pl.ds(pl.multiple_of(who * rows, rows), rows)]
        return remote(blk, blk, mos.at[k], mor.at[k], (b, (g + k) % ga))

    def m_relay(c, k, who):
        blk = mbuf.at[1, pl.ds(pl.multiple_of(who * rows + c * cr, cr), cr)]
        return remote(blk, blk, mrs.at[c, k], mrr.at[c, k], (b, (g + k) % ga))

    def accumulate(h, p):
        step = 512

        @pl.loop(0, cols // step)
        def _(c):
            at = pl.ds(pl.multiple_of(c * step, step), step)
            low = pl.ds(pl.multiple_of(p * kc, kc), kc)
            s[h, :, at] += jnp.dot(wbuf[p], mbuf[h, low, at], preferred_element_type=jnp.float32)

    load_x = pltpu.make_async_copy(w_ref.at[pl.ds(pl.multiple_of((1 - x) * half, half), half)], wx, lsem.at[0])
    load_w = pltpu.make_async_copy(w_ref.at[pl.ds(pl.multiple_of(x * half, half), half)], wbuf.at[b], lsem.at[1])
    load_m = pltpu.make_async_copy(m_ref, mbuf.at[0, pl.ds(pl.multiple_of(g * rows, rows), rows)], lsem.at[2])
    load_x.start()
    load_w.start()
    load_m.start()
    load_x.wait()
    w_x().start()
    load_w.wait()
    w_y(0, 0, y).start()
    for k in range(1, nz):
        w_z(0, k).start()
    load_m.wait()
    for c in range(CHUNKS):
        m_x(c).start()
    for k in range(1, ga):
        m_own(k, g).start()
    s[...] = jnp.zeros_like(s)

    steps = 2 * nz
    done = 0
    for step in range(steps):
        k, kind = step // 2, step % 2
        if step == 1:
            w_x_in().wait_recv()
            for kk in range(1, nz):
                w_z(1, kk).start()
        elif k > 0:
            w_z_in(kind, k).wait_recv()
        if step > 0:
            w_y(kind, k, y).start()
        if step == 0:
            for kk in range(1, ga):
                m_own(kk, (g + ga - kk) % ga).wait_recv()
        accumulate(0, piece((z + nz - k) % nz, y, side(kind)))
        w_y(kind, k, 1 - y).wait_recv()
        while done * steps < (step + 1) * CHUNKS and done < CHUNKS:
            m_x(done).wait_recv()
            for kk in range(1, ga):
                m_relay(done, kk, g).start()
            done += 1
        accumulate(0, piece((z + nz - k) % nz, 1 - y, side(kind)))

    for c in range(CHUNKS):
        for kk in range(1, ga):
            m_relay(c, kk, (g + ga - kk) % ga).wait_recv()

    @pl.loop(0, n)
    def _(p):
        accumulate(1, p)

    mine = pl.ds(pl.multiple_of(g * rows + x * half, half), half)
    wide = 4 * bw
    for h in range(2):

        @pl.loop(0, cols // wide)
        def _(q):
            at = pl.ds(pl.multiple_of(q * wide, wide), wide)
            left = mbuf[h, mine, at]
            image = s[h, :, at]
            high = image.astype(jnp.bfloat16)
            low = (image - high.astype(jnp.float32)).astype(jnp.bfloat16)
            dims = (((0,), (0,)), ((), ()))
            both = lax.dot_general(left, high, dims, preferred_element_type=jnp.float32)
            both += lax.dot_general(left, low, dims, preferred_element_type=jnp.float32)
            for t in range(4):
                a_ref[h, q * 4 + t] = both[t * bw : (t + 1) * bw, t * bw : (t + 1) * bw]

    w_x().wait_send()
    for kind in range(2):
        for k in range(nz):
            w_y(kind, k, y).wait_send()
            if k > 0:
                w_z(kind, k).wait_send()
    for c in range(CHUNKS):
        m_x(c).wait_send()
        for k in range(1, ga):
            m_relay(c, k, g).wait_send()
    for k in range(1, ga):
        m_own(k, g).wait_send()


def intersections(n, ga, bw, elements, screening):
    rows, cols = elements.shape
    half, kc, nz = rows // 2, screening.shape[1], n // 4
    dma = pltpu.SemaphoreType.DMA
    return pl.pallas_call(
        functools.partial(sigma_kernel, n, ga, bw),
        out_shape=jax.ShapeDtypeStruct((2, cols // bw, bw, bw), jnp.float32),
        in_specs=[pl.BlockSpec(memory_space=pl.ANY)] * 2,
        out_specs=pl.BlockSpec(memory_space=pltpu.VMEM),
        scratch_shapes=[
            pltpu.VMEM((2, rows * ga, cols), jnp.bfloat16),
            pltpu.VMEM((n, half, kc), jnp.bfloat16),
            pltpu.VMEM((half, kc), jnp.bfloat16),
            pltpu.VMEM((2, half, cols), jnp.float32),
            dma((3,)),
            dma,
            dma,
            dma((CHUNKS,)),
            dma((CHUNKS,)),
            dma((ga,)),
            dma((ga,)),
            dma((CHUNKS, ga)),
            dma((CHUNKS, ga)),
            dma((2, nz)),
            dma((2, nz)),
            dma((2, nz)),
            dma((2, nz)),
        ],
        compiler_params=pltpu.CompilerParams(has_side_effects=True, vmem_limit_bytes=60 * 2**20),
        name="pair_screen",
    )(elements, screening)


def band_weights(energies, frequencies, qp_index, occupied, offsets, band_count):
    position = jnp.arange(energies.shape[0], dtype=jnp.int32)
    signed = jnp.where(occupied == 1, -energies, energies)
    onehot = (qp_index[:, None] == position[None, :]).astype(jnp.float32)
    state_level = jnp.sum(onehot * signed[None, :], axis=1)
    band_level = jnp.stack([lax.dynamic_slice_in_dim(signed, o, band_count, 0) for o in offsets])
    detuning = state_level[None, None, :] - band_level[:, :, None]
    imag_freq = frequencies[:, None, None, None]
    modulus = detuning[None] ** 2 + imag_freq**2
    return detuning[None] / modulus, -imag_freq / modulus


def shards(n, ga, elements, screening, energies, frequencies, qp_index, occupied):
    states = qp_index.shape[0]
    bands = elements.shape[1] // (2 * states)
    cross = intersections(n, ga, 2 * states, elements, screening)
    real = cross[:, :, :states, :states] + cross[:, :, states:, states:]
    imag = cross[:, :, :states, states:] - cross[:, :, states:, :states]
    b = lax.axis_index("blk")
    offsets = [b * bands, (b + 1 - 2 * (b % 2)) * bands]
    wr, wi = band_weights(energies, frequencies, qp_index, occupied, offsets, bands)
    wr, wi = wr[..., None], wi[..., None]
    sigma_real = jnp.sum(wr * real[None] - wi * imag[None], axis=(1, 2))
    sigma_imag = jnp.sum(wr * imag[None] + wi * real[None], axis=(1, 2))
    total = lax.psum(jnp.stack([sigma_real, sigma_imag]), ("blk", "ga"))
    return total / (elements.shape[0] * ga)


def solution(mesh):
    placed = (P("ga", "blk"), P("ga", "blk"), P(), P(), P(), P())
    body = functools.partial(shards, mesh.shape["blk"], mesh.shape["ga"])
    return jax.shard_map(body, mesh=mesh, in_specs=placed, out_specs=P(), check_vma=False)
```

```python
import functools

import jax
import jax.numpy as jnp
from jax import lax
from jax.experimental import pallas as pl
from jax.experimental.pallas import tpu as pltpu
from jax.sharding import PartitionSpec as P

MESH = pl.DeviceIdType.MESH


def sigma_kernel(
    n, ga, bw, m_ref, w_ref, a_ref, mbuf, wbuf, wx, s, lsem,
    wxs, wxr, mxs, mxr, mos, mor, mrs, mrr, wzs, wzr, wys, wyr,
):
    rows, cols = m_ref.shape
    half = rows // 2
    kc = w_ref.shape[1]
    nz = n // 4
    layers = nz // ga
    chunks = 4 * layers
    cr = rows // chunks
    b, g = lax.axis_index("blk"), lax.axis_index("ga")
    x, y, z = b % 2, (b // 2) % 2, b // 4
    px = b + 1 - 2 * x
    py = b + 2 - 4 * y

    def remote(src, dst, ss, rs, dev):
        return pltpu.make_async_remote_copy(
            src_ref=src, dst_ref=dst, send_sem=ss, recv_sem=rs, device_id=dev, device_id_type=MESH
        )

    def piece(zz, yy, xx):
        return zz * 4 + yy * 2 + xx

    def side(kind):
        return x if kind == 0 else 1 - x

    def w_x():
        return remote(wx, wbuf.at[b], wxs, wxr, (px, g))

    def w_x_in():
        return remote(wx, wbuf.at[px], wxs, wxr, (px, g))

    def w_z(kind, k):
        blk = wbuf.at[piece(z, y, side(kind))]
        return remote(blk, blk, wzs.at[kind, k], wzr.at[kind, k], (piece((z + k) % nz, y, x), g))

    def w_z_in(kind, k):
        blk = wbuf.at[piece((z + nz - k) % nz, y, side(kind))]
        return remote(blk, blk, wzs.at[kind, k], wzr.at[kind, k], (piece((z + k) % nz, y, x), g))

    def w_y(kind, k, row):
        blk = wbuf.at[piece((z + nz - k) % nz, row, side(kind))]
        return remote(blk, blk, wys.at[kind, k], wyr.at[kind, k], (py, g))

    def layer(who, u):
        start = jnp.where(z // layers == who, z % layers, layers - 1)
        return who * layers + (start + layers - u) % layers

    def m_rows(who, c):
        return pl.ds(pl.multiple_of((layer(who, c // 4) * 4 + c % 4) * cr, cr), cr)

    def m_x(c):
        at = m_rows(g, c)
        return remote(mbuf.at[0, at], mbuf.at[1, at], mxs.at[c], mxr.at[c], (px, g))

    def m_own(k, who):
        blk = mbuf.at[0, pl.ds(pl.multiple_of(who * rows, rows), rows)]
        return remote(blk, blk, mos.at[k], mor.at[k], (b, (g + k) % ga))

    def m_relay(c, k, who):
        blk = mbuf.at[1, m_rows(who, c)]
        return remote(blk, blk, mrs.at[c, k], mrr.at[c, k], (b, (g + k) % ga))

    def accumulate(h, p):
        step = 512

        @pl.loop(0, cols // step)
        def _(c):
            at = pl.ds(pl.multiple_of(c * step, step), step)
            low = pl.ds(pl.multiple_of(p * kc, kc), kc)
            s[h, :, at] += jnp.dot(wbuf[p], mbuf[h, low, at], preferred_element_type=jnp.float32)

    def accumulate_layer(zz):
        step = 512

        @pl.loop(0, cols // step)
        def _(c):
            at = pl.ds(pl.multiple_of(c * step, step), step)
            total = s[1, :, at]
            for t in range(4):
                low = pl.ds(pl.multiple_of((zz * 4 + t) * kc, kc), kc)
                total += jnp.dot(wbuf[zz * 4 + t], mbuf[1, low, at], preferred_element_type=jnp.float32)
            s[1, :, at] = total

    def early():
        for c in range(4):
            for kk in range(1, ga):
                m_relay(c, kk, (g + ga - kk) % ga).wait_recv()

    def first(who, zz):
        return who * layers + (zz % layers if zz // layers == who else layers - 1)

    reach = max((zz - first(who, zz)) % nz for zz in range(nz) for who in range(ga))

    load_x = pltpu.make_async_copy(w_ref.at[pl.ds(pl.multiple_of((1 - x) * half, half), half)], wx, lsem.at[0])
    load_w = pltpu.make_async_copy(w_ref.at[pl.ds(pl.multiple_of(x * half, half), half)], wbuf.at[b], lsem.at[1])
    load_m = pltpu.make_async_copy(m_ref, mbuf.at[0, pl.ds(pl.multiple_of(g * rows, rows), rows)], lsem.at[2])
    load_x.start()
    load_w.start()
    load_m.start()
    load_x.wait()
    w_x().start()
    load_w.wait()
    w_y(0, 0, y).start()
    for k in range(1, nz):
        w_z(0, k).start()
    load_m.wait()
    for c in range(chunks):
        m_x(c).start()
    for k in range(1, ga):
        m_own(k, g).start()
    s[...] = jnp.zeros_like(s)

    steps = 2 * nz
    done = 0
    swept = 0
    for step in range(steps):
        k, kind = step // 2, step % 2
        if step == 1:
            w_x_in().wait_recv()
            for kk in range(1, nz):
                w_z(1, kk).start()
        elif k > 0:
            w_z_in(kind, k).wait_recv()
        if step > 0:
            w_y(kind, k, y).start()
        if step == 0:
            for kk in range(1, ga):
                m_own(kk, (g + ga - kk) % ga).wait_recv()
        accumulate(0, piece((z + nz - k) % nz, y, side(kind)))
        w_y(kind, k, 1 - y).wait_recv()
        while done * steps < (step + 1) * chunks and done < chunks:
            m_x(done).wait_recv()
            for kk in range(1, ga):
                m_relay(done, kk, g).start()
            done += 1
        accumulate(0, piece((z + nz - k) % nz, 1 - y, side(kind)))
        if step == 2 * reach + 2:
            early()
        if step >= 2 * reach + 2 and done >= 4:
            while swept < ga and swept * (steps - 2 * reach - 2) < (step - 2 * reach - 1) * ga:
                accumulate_layer(layer(swept, 0))
                swept += 1

    if 2 * reach + 2 >= steps:
        early()
    for c in range(4, chunks):
        for kk in range(1, ga):
            m_relay(c, kk, (g + ga - kk) % ga).wait_recv()

    for who in range(swept, ga):
        accumulate_layer(layer(who, 0))
    for who in range(ga):
        for u in range(1, layers):
            accumulate_layer(layer(who, u))

    mine = pl.ds(pl.multiple_of(g * rows + x * half, half), half)
    wide = 4 * bw
    for h in range(2):

        @pl.loop(0, cols // wide)
        def _(q):
            at = pl.ds(pl.multiple_of(q * wide, wide), wide)
            left = mbuf[h, mine, at]
            image = s[h, :, at]
            high = image.astype(jnp.bfloat16)
            low = (image - high.astype(jnp.float32)).astype(jnp.bfloat16)
            dims = (((0,), (0,)), ((), ()))
            both = lax.dot_general(left, high, dims, preferred_element_type=jnp.float32)
            both += lax.dot_general(left, low, dims, preferred_element_type=jnp.float32)
            for t in range(4):
                a_ref[h, q * 4 + t] = both[t * bw : (t + 1) * bw, t * bw : (t + 1) * bw]

    w_x().wait_send()
    for kind in range(2):
        for k in range(nz):
            w_y(kind, k, y).wait_send()
            if k > 0:
                w_z(kind, k).wait_send()
    for c in range(chunks):
        m_x(c).wait_send()
        for k in range(1, ga):
            m_relay(c, k, g).wait_send()
    for k in range(1, ga):
        m_own(k, g).wait_send()


def intersections(n, ga, bw, elements, screening):
    rows, cols = elements.shape
    half, kc, nz = rows // 2, screening.shape[1], n // 4
    chunks = 4 * (nz // ga)
    dma = pltpu.SemaphoreType.DMA
    return pl.pallas_call(
        functools.partial(sigma_kernel, n, ga, bw),
        out_shape=jax.ShapeDtypeStruct((2, cols // bw, bw, bw), jnp.float32),
        in_specs=[pl.BlockSpec(memory_space=pl.ANY)] * 2,
        out_specs=pl.BlockSpec(memory_space=pltpu.VMEM),
        scratch_shapes=[
            pltpu.VMEM((2, rows * ga, cols), jnp.bfloat16),
            pltpu.VMEM((n, half, kc), jnp.bfloat16),
            pltpu.VMEM((half, kc), jnp.bfloat16),
            pltpu.VMEM((2, half, cols), jnp.float32),
            dma((3,)),
            dma,
            dma,
            dma((chunks,)),
            dma((chunks,)),
            dma((ga,)),
            dma((ga,)),
            dma((chunks, ga)),
            dma((chunks, ga)),
            dma((2, nz)),
            dma((2, nz)),
            dma((2, nz)),
            dma((2, nz)),
        ],
        compiler_params=pltpu.CompilerParams(has_side_effects=True, vmem_limit_bytes=60 * 2**20),
        name="pair_screen",
    )(elements, screening)


def sum_kernel(n, ga, part_ref, out_ref, inbox, sem):
    count = n * ga
    me = lax.axis_index("blk") * ga + lax.axis_index("ga")

    def remote(src, dst, phase, k):
        to = (me + k) % count
        return pltpu.make_async_remote_copy(
            src_ref=src, dst_ref=dst, send_sem=sem.at[phase, 0], recv_sem=sem.at[phase, 1],
            device_id=(to // ga, to % ga), device_id_type=MESH,
        )

    @pl.loop(1, count)
    def _(k):
        remote(part_ref.at[(me + k) % count], inbox.at[k - 1], 0, k).start()

    remote(inbox, inbox, 0, 1).wait_recv()
    out_ref[me] = part_ref[me] + jnp.sum(inbox[...], axis=0)

    @pl.loop(1, count)
    def _(k):
        remote(out_ref.at[me], out_ref.at[me], 1, k).start()

    remote(inbox, inbox, 0, 1).wait_send()
    remote(inbox, inbox, 1, 1).wait_recv()
    remote(inbox, inbox, 1, 1).wait_send()


def sum_everywhere(n, ga, part):
    count = n * ga
    width = part.size // count
    vmem = pl.BlockSpec(memory_space=pltpu.VMEM)
    return pl.pallas_call(
        functools.partial(sum_kernel, n, ga),
        out_shape=jax.ShapeDtypeStruct((count, 1, width), jnp.float32),
        in_specs=[vmem],
        out_specs=vmem,
        scratch_shapes=[pltpu.VMEM((count - 1, 1, width), jnp.float32), pltpu.SemaphoreType.DMA((2, 2))],
        compiler_params=pltpu.CompilerParams(has_side_effects=True),
        name="sum_all",
    )(part.reshape(count, 1, width)).reshape(part.shape)


def band_weights(energies, frequencies, qp_index, occupied, offsets, band_count):
    position = jnp.arange(energies.shape[0], dtype=jnp.int32)
    signed = jnp.where(occupied == 1, -energies, energies)
    onehot = (qp_index[:, None] == position[None, :]).astype(jnp.float32)
    state_level = jnp.sum(onehot * signed[None, :], axis=1)
    band_level = jnp.stack([lax.dynamic_slice_in_dim(signed, o, band_count, 0) for o in offsets])
    detuning = state_level[None, None, :] - band_level[:, :, None]
    imag_freq = frequencies[:, None, None, None]
    modulus = detuning[None] ** 2 + imag_freq**2
    return detuning[None] / modulus, -imag_freq / modulus


def shards(n, ga, elements, screening, energies, frequencies, qp_index, occupied):
    states = qp_index.shape[0]
    bands = elements.shape[1] // (2 * states)
    cross = intersections(n, ga, 2 * states, elements, screening)
    real = cross[:, :, :states, :states] + cross[:, :, states:, states:]
    imag = cross[:, :, :states, states:] - cross[:, :, states:, :states]
    b = lax.axis_index("blk")
    offsets = [b * bands, (b + 1 - 2 * (b % 2)) * bands]
    wr, wi = band_weights(energies, frequencies, qp_index, occupied, offsets, bands)
    wr, wi = wr[..., None], wi[..., None]
    sigma_real = jnp.sum(wr * real[None] - wi * imag[None], axis=(1, 2))
    sigma_imag = jnp.sum(wr * imag[None] + wi * real[None], axis=(1, 2))
    share = jnp.stack([sigma_real, sigma_imag]) / (elements.shape[0] * ga)
    return sum_everywhere(n, ga, share)


def solution(mesh):
    placed = (P("ga", "blk"), P("ga", "blk"), P(), P(), P(), P())
    body = functools.partial(shards, mesh.shape["blk"], mesh.shape["ga"])
    return jax.shard_map(body, mesh=mesh, in_specs=placed, out_specs=P(), check_vma=False)
```
